128 devices in a mesh: rows: 8 (over z, core), cols: 4 (over y), slabs: 4 (over x).
Axes of the slice: x: 4, y: 4, z: 4, core: 2. Of those that a mesh axis runs over, the one named last changes fastest.
Arguments:
- tracer: float32 [32, 256, 384, 128], P('rows', 'cols', 'slabs'), may hold values from 0.2 to 1.8
- crowding: float32 [32, 256, 384, 128], P('rows', 'cols', 'slabs'), may hold values from 0.5 to 2
Outputs:
- tracer_end: float32 [32, 256, 384, 128], P('rows', 'cols', 'slabs')
The draws below stay inside these ranges and needn't reach their ends.
All inputs are finite; a program needn't handle non-finite values.
Results may differ from the reference program's by a relative error of at most 0.00002.
Values sent between devices are 32-bit elements.
A program may use at most 448 MiB of HBM per device.

```python
import jax
import jax.numpy as jnp
from jax import lax

GRID_Y = 32
GRID_X = 256
GRID_Z = 384
SPECIES = 128
STEPS = 4


def block_levels(key, shape, cuts, smallest, top_value):
    loudness = 1.0
    for dim, shards_of in cuts:
        steps = jax.random.uniform(jax.random.fold_in(jax.random.fold_in(key, 6), dim), (shards_of,), jnp.float32, smallest / len(cuts), top_value / len(cuts))
        loudness = loudness * jnp.repeat(jnp.exp(steps), shape[dim] // shards_of).reshape((-1,) + (1,) * (len(shape) - 1 - dim))
    return loudness


def setup_inputs(seed: int = 0) -> dict:
    key_of = jax.random.split(jax.random.key(seed), 3)
    return {
        "tracer": jnp.clip(0.2 + 1.5999999 * jax.random.uniform(key_of[0], (GRID_Y, GRID_X, GRID_Z, SPECIES), jnp.float32) ** block_levels(key_of[0], (GRID_Y, GRID_X, GRID_Z, SPECIES), ((0, 8), (1, 4), (2, 4)), -0.2, 0.2), 0.2, 1.8),
        "crowding": jnp.clip(0.5 + 1.5 * jax.random.uniform(key_of[1], (GRID_Y, GRID_X, GRID_Z, SPECIES), jnp.float32) ** block_levels(key_of[1], (GRID_Y, GRID_X, GRID_Z, SPECIES), ((0, 8), (1, 4), (2, 4)), -0.2, 0.2), 0.5, 2.0),
    }


def inner_cells(values, dims):
    for dim in dims:
        values = lax.slice_in_dim(values, 1, values.shape[dim] - 1, axis=dim)
    return values


def side_cells(values, dim, start, dims):
    others = [other for other in dims if other != dim]
    values = inner_cells(values, others)
    return lax.slice_in_dim(values, start, start + values.shape[dim] - 2, axis=dim)


def advance(padded, crowding):
    middle = inner_cells(padded, (0, 1, 2))
    lower = [side_cells(padded, dim, 0, (0, 1, 2)) for dim in (0, 1, 2)]
    upper = [side_cells(padded, dim, 2, (0, 1, 2)) for dim in (0, 1, 2)]
    spread = lower[0] + upper[0] + lower[1] + upper[1] + lower[2] + upper[2] - 6.0 * middle
    return middle + 0.1 * spread + 0.2 * middle * (1.0 - middle * crowding)


def reference(tracer, crowding):
    for step in range(STEPS):
        tracer = advance(jnp.pad(tracer, ((1, 1), (1, 1), (1, 1), (0, 0)), mode="constant"), crowding)
    return tracer
```

```python
import functools

import jax
import jax.numpy as jnp
from jax import lax
from jax.experimental import pallas as pl
from jax.experimental.pallas import tpu as pltpu
from jax.sharding import PartitionSpec as P

STEPS = 4
CHUNKS = 8
MESH = pl.DeviceIdType.MESH
VMEM_LIMIT = 48 * 1024 * 1024


def kernel(sizes, tracer, crowding, out, field, far_in, near_in, slab_in, slab_out,
           load_sem, far_send, far_recv, near_send, near_recv,
           cols_send, cols_recv, slab_send, slab_recv):
    layers, lines, depth, _ = tracer.shape
    per_chunk = lines // CHUNKS
    tiles = depth // 8
    rows_n, cols_n, slabs_n = sizes
    r, q, s = lax.axis_index("rows"), lax.axis_index("cols"), lax.axis_index("slabs")
    core = lax.rem(r, 2)
    step_up = 1 - 2 * core
    first = (layers - 1) * core

    def layer(d):
        return first + step_up * d

    far_row = r - step_up
    near_row = r + step_up
    has_far = jnp.logical_and(far_row >= 0, far_row < rows_n)
    around = (
        ("cols", q, cols_n),
        ("slabs", s, slabs_n),
    )

    loads = [
        pltpu.make_async_copy(tracer, field.at[0, :, pl.ds(1, lines)], load_sem.at[0]),
        pltpu.make_async_copy(crowding, out, load_sem.at[1]),
    ]
    loads[0].start()

    barrier = pltpu.get_barrier_semaphore()
    greeted = jnp.int32(1)
    pl.semaphore_signal(barrier, inc=1, device_id={"rows": near_row}, device_id_type=MESH)

    @pl.when(has_far)
    def _():
        pl.semaphore_signal(barrier, inc=1, device_id={"rows": far_row}, device_id_type=MESH)

    greeted = greeted + has_far.astype(jnp.int32)
    for axis, me, n in around:
        @pl.when(me > 0)
        def _():
            pl.semaphore_signal(barrier, inc=1, device_id={axis: me - 1}, device_id_type=MESH)

        @pl.when(me < n - 1)
        def _():
            pl.semaphore_signal(barrier, inc=1, device_id={axis: me + 1}, device_id_type=MESH)

        greeted = greeted + (me > 0).astype(jnp.int32) + (me < n - 1).astype(jnp.int32)
    pl.semaphore_wait(barrier, greeted)

    def far_copy(par, c, source):
        part = pl.ds(c * per_chunk, per_chunk)
        return pltpu.make_async_remote_copy(
            src_ref=source, dst_ref=far_in.at[par, part],
            send_sem=far_send.at[par, c], recv_sem=far_recv.at[par, c],
            device_id={"rows": far_row}, device_id_type=MESH,
        )

    def far_source(par, c):
        return field.at[par, layer(0), pl.ds(1 + c * per_chunk, per_chunk)]

    def near_copy(par, source):
        return pltpu.make_async_remote_copy(
            src_ref=source, dst_ref=near_in.at[par],
            send_sem=near_send.at[par], recv_sem=near_recv.at[par],
            device_id={"rows": near_row}, device_id_type=MESH,
        )

    def near_source(par):
        return field.at[par, layer(layers - 1), pl.ds(1, lines)]

    def cols_copy(par, side, source):
        return pltpu.make_async_remote_copy(
            src_ref=source, dst_ref=field.at[par, :, (lines + 1) * (1 - side)],
            send_sem=cols_send.at[par, side], recv_sem=cols_recv.at[par, side],
            device_id={"cols": q - 1 + 2 * side}, device_id_type=MESH,
        )

    def cols_source(par, side):
        return field.at[par, :, 1 + (lines - 1) * side]

    def slab_copy(par, side):
        return pltpu.make_async_remote_copy(
            src_ref=slab_out.at[par, side], dst_ref=slab_in.at[par, 1 - side],
            send_sem=slab_send.at[par, side], recv_sem=slab_recv.at[par, side],
            device_id={"slabs": s - 1 + 2 * side}, device_id_type=MESH,
        )

    def has(me, n, side):
        return me > 0 if side == 0 else me < n - 1

    @pl.when(has_far)
    def _():
        @pl.loop(0, CHUNKS)
        def _(c):
            far_copy(0, c, tracer.at[layer(0), pl.ds(c * per_chunk, per_chunk)]).start()

    near_copy(0, tracer.at[layer(layers - 1)]).start()
    for side in (0, 1):
        @pl.when(has(q, cols_n, side))
        def _():
            cols_copy(0, side, tracer.at[:, (lines - 1) * side]).start()
    loads[1].start()

    for side in (0, 1):
        @pl.when(jnp.logical_not(has(q, cols_n, side)))
        def _():
            for par in (0, 1):
                field[par, :, (lines + 1) * side] = jnp.zeros((layers, depth, 128), jnp.float32)

        @pl.when(jnp.logical_not(has(s, slabs_n, side)))
        def _():
            for par in (0, 1):
                @pl.loop(0, layers)
                def _(i):
                    slab_in[par, side, i] = jnp.zeros((lines, 128), jnp.float32)

    @pl.when(jnp.logical_not(has_far))
    def _():
        for par in (0, 1):
            @pl.loop(0, lines)
            def _(j):
                far_in[par, j] = jnp.zeros((depth, 128), jnp.float32)

    loads[0].wait()

    @pl.loop(0, layers)
    def _(i):
        @pl.loop(0, lines)
        def _(j):
            slab_out[0, 0, i, pl.ds(j, 1), :] = field[0, i, j + 1, 0:1, :]
            slab_out[0, 1, i, pl.ds(j, 1), :] = field[0, i, j + 1, depth - 1:depth, :]

    for side in (0, 1):
        @pl.when(has(s, slabs_n, side))
        def _():
            slab_copy(0, side).start()
    loads[1].wait()

    row = lax.broadcasted_iota(jnp.int32, (8, 128), 0)

    def advance(t, d, start, count):
        par, last = t % 2, t == STEPS - 1
        here = layer(d)

        @pl.loop(start, start + count)
        def _(j):
            below = slab_in[par, 0, here, pl.ds(j, 1), :]
            above = slab_in[par, 1, here, pl.ds(j, 1), :]
            for k in range(tiles):
                part = pl.ds(8 * k, 8)
                mid = field[par, here, j + 1, part, :]
                if k == 0:
                    lower = jnp.where(row == 0, below, pltpu.roll(mid, 1, 0))
                else:
                    lower = field[par, here, j + 1, pl.ds(8 * k - 1, 8), :]
                if k == tiles - 1:
                    upper = jnp.where(row == 7, above, pltpu.roll(mid, 7, 0))
                else:
                    upper = field[par, here, j + 1, pl.ds(8 * k + 1, 8), :]
                outer = far_in[par, j, part, :] if d == 0 else field[par, layer(d - 1), j + 1, part, :]
                inner = near_in[par, j, part, :] if d == layers - 1 else field[par, layer(d + 1), j + 1, part, :]
                spread = (
                    (lower + upper)
                    + (field[par, here, j, part, :] + field[par, here, j + 2, part, :])
                    + (outer + inner)
                )
                crowd = out[here, j, part, :]
                new = 0.1 * spread + mid * (0.6 - 0.2 * (mid * crowd))
                if last:
                    out[here, j, part, :] = new
                else:
                    field[1 - par, here, j + 1, part, :] = new
                    if k == 0:
                        slab_out[1 - par, 0, here, pl.ds(j, 1), :] = new[0:1]
                    if k == tiles - 1:
                        slab_out[1 - par, 1, here, pl.ds(j, 1), :] = new[7:8]

    for t in range(STEPS):
        par, last = t % 2, t == STEPS - 1
        nxt = 1 - par
        near_copy(par, near_source(par)).wait_recv()
        for side in (0, 1):
            @pl.when(has(q, cols_n, 1 - side))
            def _():
                cols_copy(par, side, cols_source(par, side)).wait_recv()

            @pl.when(has(s, slabs_n, 1 - side))
            def _():
                slab_copy(par, side).wait_recv()
        if t > 0:
            near_copy(nxt, near_source(nxt)).wait_send()
            for side in (0, 1):
                @pl.when(has(q, cols_n, side))
                def _():
                    cols_copy(nxt, side, cols_source(nxt, side)).wait_send()

                @pl.when(has(s, slabs_n, side))
                def _():
                    slab_copy(nxt, side).wait_send()
        for d in range(layers - 1, 0, -1):
            advance(t, d, 0, lines)
        if not last:
            near_copy(nxt, near_source(nxt)).start()

        @pl.loop(0, CHUNKS)
        def _(c):
            @pl.when(has_far)
            def _():
                far_copy(par, c, far_source(par, c)).wait_recv()
                if t > 0:
                    far_copy(nxt, c, far_source(nxt, c)).wait_send()

            advance(t, 0, c * per_chunk, per_chunk)
            if not last:
                @pl.when(has_far)
                def _():
                    far_copy(nxt, c, far_source(nxt, c)).start()
        if not last:
            for side in (0, 1):
                @pl.when(has(q, cols_n, side))
                def _():
                    cols_copy(nxt, side, cols_source(nxt, side)).start()

                @pl.when(has(s, slabs_n, side))
                def _():
                    slab_copy(nxt, side).start()

    par = (STEPS - 1) % 2
    near_copy(par, near_source(par)).wait_send()
    for side in (0, 1):
        @pl.when(has(q, cols_n, side))
        def _():
            cols_copy(par, side, cols_source(par, side)).wait_send()

        @pl.when(has(s, slabs_n, side))
        def _():
            slab_copy(par, side).wait_send()

    @pl.when(has_far)
    def _():
        @pl.loop(0, CHUNKS)
        def _(c):
            far_copy(par, c, far_source(par, c)).wait_send()


def solution(mesh):
    sizes = tuple(mesh.shape[axis] for axis in ("rows", "cols", "slabs"))

    def on_device(tracer, crowding):
        layers, lines, depth, lanes = tracer.shape
        dma = pltpu.SemaphoreType.DMA
        return pl.pallas_call(
            functools.partial(kernel, sizes),
            out_shape=pltpu.VMEM(tracer.shape, jnp.float32),
            in_specs=[pl.BlockSpec(memory_space=pl.ANY)] * 2,
            out_specs=pl.BlockSpec(memory_space=pltpu.VMEM),
            scratch_shapes=[
                pltpu.VMEM((2, layers, lines + 2, depth, lanes), jnp.float32),
                pltpu.VMEM((2, lines, depth, lanes), jnp.float32),
                pltpu.VMEM((2, lines, depth, lanes), jnp.float32),
                pltpu.VMEM((2, 2, layers, lines, lanes), jnp.float32),
                pltpu.VMEM((2, 2, layers, lines, lanes), jnp.float32),
                dma((2,)),
                dma((2, CHUNKS)), dma((2, CHUNKS)),
                dma((2,)), dma((2,)),
                dma((2, 2)), dma((2, 2)),
                dma((2, 2)), dma((2, 2)),
            ],
            compiler_params=pltpu.CompilerParams(
                collective_id=0, has_side_effects=True, vmem_limit_bytes=VMEM_LIMIT,
            ),
        )(tracer, crowding)

    placed = P("rows", "cols", "slabs", None)
    return jax.shard_map(on_device, mesh=mesh, in_specs=(placed, placed), out_specs=placed, check_vma=False)
```

```python
import functools

import jax
import jax.numpy as jnp
from jax import lax
from jax.experimental import pallas as pl
from jax.experimental.pallas import tpu as pltpu
from jax.sharding import PartitionSpec as P

STEPS = 4
PARTS = ((32, 32), (32, 32), (32, 32), (32, 16, 8, 6, 2))
MOST = max(map(len, PARTS))
MESH = pl.DeviceIdType.MESH
VMEM_LIMIT = 48 * 1024 * 1024


def kernel(sizes, tracer, crowding, out, field, far_in, near_in, slab_in, slab_out,
           all_in, load_sem, far_send, far_recv, near_send, near_recv,
           cols_send, cols_recv, slab_send, slab_recv):
    layers, lines, depth, _ = tracer.shape
    tiles = depth // 8
    rows_n, cols_n, slabs_n = sizes
    r, q, s = lax.axis_index("rows"), lax.axis_index("cols"), lax.axis_index("slabs")
    core = lax.rem(r, 2)
    step_up = 1 - 2 * core
    first = (layers - 1) * core

    def layer(d):
        return first + step_up * d

    far_row = r - step_up
    near_row = r + step_up
    has_far = jnp.logical_and(far_row >= 0, far_row < rows_n)
    around = (
        ("cols", q, cols_n),
        ("slabs", s, slabs_n),
    )

    def spans(t):
        start = 0
        for p, count in enumerate(PARTS[t]):
            yield p, start, count
            start += count

    loads = [
        pltpu.make_async_copy(tracer, field.at[0, :, pl.ds(1, lines)], load_sem.at[0]),
        pltpu.make_async_copy(crowding, out, load_sem.at[1]),
    ]

    barrier = pltpu.get_barrier_semaphore()

    def greet(there, target):
        @pl.when(there)
        def _():
            pl.semaphore_signal(barrier, inc=1, device_id=target, device_id_type=MESH)

    greet(has_far, {"rows": far_row})
    greet(core == 0, {"rows": near_row})
    beside = jnp.int32(0)
    for axis, me, n in around:
        for there, other in ((me > 0, me - 1), (me < n - 1, me + 1)):
            greet(there, {"rows": r + 1 - core, axis: other})
            beside = beside + there.astype(jnp.int32)
    greeted = has_far.astype(jnp.int32) + core * (1 + 2 * beside)

    @pl.when(greeted > 0)
    def _():
        pl.semaphore_wait(barrier, greeted)

    def far_copy(t, p, start, count):
        par = t % 2
        source = tracer.at[layer(0), pl.ds(start, count)] if t == 0 else field.at[par, layer(0), pl.ds(1 + start, count)]
        return pltpu.make_async_remote_copy(
            src_ref=source, dst_ref=far_in.at[par, pl.ds(start, count)],
            send_sem=far_send.at[par, p], recv_sem=far_recv.at[par, p],
            device_id={"rows": far_row}, device_id_type=MESH,
        )

    def near_copy(par, source):
        return pltpu.make_async_remote_copy(
            src_ref=source, dst_ref=near_in.at[par],
            send_sem=near_send.at[par], recv_sem=near_recv.at[par],
            device_id={"rows": near_row}, device_id_type=MESH,
        )

    def near_source(par):
        return field.at[par, layer(layers - 1), pl.ds(1, lines)]

    def cols_copy(par, side, source):
        return pltpu.make_async_remote_copy(
            src_ref=source, dst_ref=field.at[par, :, (lines + 1) * (1 - side)],
            send_sem=cols_send.at[par, side], recv_sem=cols_recv.at[par, side],
            device_id={"cols": q - 1 + 2 * side}, device_id_type=MESH,
        )

    def cols_source(par, side):
        return field.at[par, :, 1 + (lines - 1) * side]

    def slab_copy(par, side):
        return pltpu.make_async_remote_copy(
            src_ref=slab_out.at[par, side], dst_ref=slab_in.at[par, 1 - side],
            send_sem=slab_send.at[par, side], recv_sem=slab_recv.at[par, side],
            device_id={"slabs": s - 1 + 2 * side}, device_id_type=MESH,
        )

    def has(me, n, side):
        return me > 0 if side == 0 else me < n - 1

    @pl.when(has_far)
    def _():
        for span in spans(0):
            far_copy(0, *span).start()

    loads[0].start()

    @pl.when(core == 1)
    def _():
        pl.semaphore_signal(all_in, inc=1, device_id={"rows": near_row}, device_id_type=MESH)

    @pl.when(core == 0)
    def _():
        pl.semaphore_wait(all_in, 1)

    near_copy(0, tracer.at[layer(layers - 1)]).start()
    for side in (0, 1):
        @pl.when(has(q, cols_n, side))
        def _():
            cols_copy(0, side, tracer.at[:, (lines - 1) * side]).start()
    loads[1].start()

    for side in (0, 1):
        @pl.when(jnp.logical_not(has(q, cols_n, side)))
        def _():
            for par in (0, 1):
                field[par, :, (lines + 1) * side] = jnp.zeros((layers, depth, 128), jnp.float32)

        @pl.when(jnp.logical_not(has(s, slabs_n, side)))
        def _():
            for par in (0, 1):
                @pl.loop(0, layers)
                def _(i):
                    slab_in[par, side, i] = jnp.zeros((lines, 128), jnp.float32)

    @pl.when(jnp.logical_not(has_far))
    def _():
        for par in (0, 1):
            @pl.loop(0, lines)
            def _(j):
                far_in[par, j] = jnp.zeros((depth, 128), jnp.float32)

    loads[0].wait()

    @pl.loop(0, layers)
    def _(i):
        @pl.loop(0, lines)
        def _(j):
            slab_out[0, 0, i, pl.ds(j, 1), :] = field[0, i, j + 1, 0:1, :]
            slab_out[0, 1, i, pl.ds(j, 1), :] = field[0, i, j + 1, depth - 1:depth, :]

    for side in (0, 1):
        @pl.when(has(s, slabs_n, side))
        def _():
            slab_copy(0, side).start()
    loads[1].wait()

    row = lax.broadcasted_iota(jnp.int32, (8, 128), 0)

    def advance(t, d, start, count):
        par, last = t % 2, t == STEPS - 1
        here = layer(d)

        @pl.loop(start, start + count)
        def _(j):
            below = slab_in[par, 0, here, pl.ds(j, 1), :]
            above = slab_in[par, 1, here, pl.ds(j, 1), :]
            for k in range(tiles):
                part = pl.ds(8 * k, 8)
                mid = field[par, here, j + 1, part, :]
                if k == 0:
                    lower = jnp.where(row == 0, below, pltpu.roll(mid, 1, 0))
                else:
                    lower = field[par, here, j + 1, pl.ds(8 * k - 1, 8), :]
                if k == tiles - 1:
                    upper = jnp.where(row == 7, above, pltpu.roll(mid, 7, 0))
                else:
                    upper = field[par, here, j + 1, pl.ds(8 * k + 1, 8), :]
                outer = far_in[par, j, part, :] if d == 0 else field[par, layer(d - 1), j + 1, part, :]
                inner = near_in[par, j, part, :] if d == layers - 1 else field[par, layer(d + 1), j + 1, part, :]
                spread = (
                    (lower + upper)
                    + (field[par, here, j, part, :] + field[par, here, j + 2, part, :])
                    + (outer + inner)
                )
                crowd = out[here, j, part, :]
                new = 0.1 * spread + mid * (0.6 - 0.2 * (mid * crowd))
                if last:
                    out[here, j, part, :] = new
                else:
                    field[1 - par, here, j + 1, part, :] = new
                    if k == 0:
                        slab_out[1 - par, 0, here, pl.ds(j, 1), :] = new[0:1]
                    if k == tiles - 1:
                        slab_out[1 - par, 1, here, pl.ds(j, 1), :] = new[7:8]

    for t in range(STEPS):
        par, last = t % 2, t == STEPS - 1
        nxt = 1 - par
        near_copy(par, near_source(par)).wait_recv()
        for side in (0, 1):
            @pl.when(has(q, cols_n, 1 - side))
            def _():
                cols_copy(par, side, cols_source(par, side)).wait_recv()

            @pl.when(has(s, slabs_n, 1 - side))
            def _():
                slab_copy(par, side).wait_recv()
        if t > 0:
            near_copy(nxt, near_source(nxt)).wait_send()
            for side in (0, 1):
                @pl.when(has(q, cols_n, side))
                def _():
                    cols_copy(nxt, side, cols_source(nxt, side)).wait_send()

                @pl.when(has(s, slabs_n, side))
                def _():
                    slab_copy(nxt, side).wait_send()
        for d in range(layers - 1, 0, -1):
            advance(t, d, 0, lines)
        if not last:
            near_copy(nxt, near_source(nxt)).start()

        if t > 0:
            @pl.when(has_far)
            def _():
                for span in spans(t - 1):
                    far_copy(t - 1, *span).wait_send()

        for p, start, count in spans(t):
            @pl.when(has_far)
            def _():
                far_copy(t, p, start, count).wait_recv()

            advance(t, 0, start, count)
            if not last:
                @pl.when(has_far)
                def _():
                    for span in spans(t + 1):
                        if start < span[1] + span[2] <= start + count:
                            far_copy(t + 1, *span).start()
        if not last:
            for side in (0, 1):
                @pl.when(has(q, cols_n, side))
                def _():
                    cols_copy(nxt, side, cols_source(nxt, side)).start()

                @pl.when(has(s, slabs_n, side))
                def _():
                    slab_copy(nxt, side).start()

    par = (STEPS - 1) % 2
    near_copy(par, near_source(par)).wait_send()
    for side in (0, 1):
        @pl.when(has(q, cols_n, side))
        def _():
            cols_copy(par, side, cols_source(par, side)).wait_send()

        @pl.when(has(s, slabs_n, side))
        def _():
            slab_copy(par, side).wait_send()

    @pl.when(has_far)
    def _():
        for span in spans(STEPS - 1):
            far_copy(STEPS - 1, *span).wait_send()


def solution(mesh):
    sizes = tuple(mesh.shape[axis] for axis in ("rows", "cols", "slabs"))

    def on_device(tracer, crowding):
        layers, lines, depth, lanes = tracer.shape
        dma = pltpu.SemaphoreType.DMA
        return pl.pallas_call(
            functools.partial(kernel, sizes),
            out_shape=pltpu.VMEM(tracer.shape, jnp.float32),
            in_specs=[pl.BlockSpec(memory_space=pl.ANY)] * 2,
            out_specs=pl.BlockSpec(memory_space=pltpu.VMEM),
            scratch_shapes=[
                pltpu.VMEM((2, layers, lines + 2, depth, lanes), jnp.float32),
                pltpu.VMEM((2, lines, depth, lanes), jnp.float32),
                pltpu.VMEM((2, lines, depth, lanes), jnp.float32),
                pltpu.VMEM((2, 2, layers, lines, lanes), jnp.float32),
                pltpu.VMEM((2, 2, layers, lines, lanes), jnp.float32),
                pltpu.SemaphoreType.REGULAR,
                dma((2,)),
                dma((2, MOST)), dma((2, MOST)),
                dma((2,)), dma((2,)),
                dma((2, 2)), dma((2, 2)),
                dma((2, 2)), dma((2, 2)),
            ],
            compiler_params=pltpu.CompilerParams(
                collective_id=0, has_side_effects=True, vmem_limit_bytes=VMEM_LIMIT,
            ),
        )(tracer, crowding)

    placed = P("rows", "cols", "slabs", None)
    return jax.shard_map(on_device, mesh=mesh, in_specs=(placed, placed), out_specs=placed, check_vma=False)
```

```python
import functools

import jax
import jax.numpy as jnp
from jax import lax
from jax.experimental import pallas as pl
from jax.experimental.pallas import tpu as pltpu
from jax.sharding import PartitionSpec as P

STEPS = 4
PARTS = ((16, 32, 16), (16, 32, 16), (16, 32, 16), (16, 32, 10, 4, 1, 1))
MOST = max(map(len, PARTS))
MESH = pl.DeviceIdType.MESH
VMEM_LIMIT = 48 * 1024 * 1024


def kernel(sizes, tracer, crowding, out, field, far_in, near_in, slab_in, slab_out,
           all_in, load_sem, far_send, far_recv, near_send, near_recv,
           cols_send, cols_recv, slab_send, slab_recv):
    layers, lines, depth, _ = tracer.shape
    tiles = depth // 8
    rows_n, cols_n, slabs_n = sizes
    r, q, s = lax.axis_index("rows"), lax.axis_index("cols"), lax.axis_index("slabs")
    core = lax.rem(r, 2)
    step_up = 1 - 2 * core
    first = (layers - 1) * core

    def layer(d):
        return first + step_up * d

    far_row = r - step_up
    near_row = r + step_up
    has_far = jnp.logical_and(far_row >= 0, far_row < rows_n)
    around = (
        ("cols", q, cols_n),
        ("slabs", s, slabs_n),
    )

    def spans(t):
        start = 0
        for p, count in enumerate(PARTS[t]):
            yield p, start, count
            start += count

    loads = [
        pltpu.make_async_copy(tracer, field.at[0, :, pl.ds(1, lines)], load_sem.at[0]),
        pltpu.make_async_copy(crowding, out, load_sem.at[1]),
    ]

    barrier = pltpu.get_barrier_semaphore()

    def greet(there, target):
        @pl.when(there)
        def _():
            pl.semaphore_signal(barrier, inc=1, device_id=target, device_id_type=MESH)

    def far_copy(t, p, start, count):
        par = t % 2
        source = tracer.at[layer(0), pl.ds(start, count)] if t == 0 else field.at[par, layer(0), pl.ds(1 + start, count)]
        return pltpu.make_async_remote_copy(
            src_ref=source, dst_ref=far_in.at[par, pl.ds(start, count)],
            send_sem=far_send.at[par, p], recv_sem=far_recv.at[par, p],
            device_id={"rows": far_row}, device_id_type=MESH,
        )

    def near_copy(par, source):
        return pltpu.make_async_remote_copy(
            src_ref=source, dst_ref=near_in.at[par],
            send_sem=near_send.at[par], recv_sem=near_recv.at[par],
            device_id={"rows": near_row}, device_id_type=MESH,
        )

    def near_source(par):
        return field.at[par, layer(layers - 1), pl.ds(1, lines)]

    def cols_copy(par, side, source):
        return pltpu.make_async_remote_copy(
            src_ref=source, dst_ref=field.at[par, :, (lines + 1) * (1 - side)],
            send_sem=cols_send.at[par, side], recv_sem=cols_recv.at[par, side],
            device_id={"cols": q - 1 + 2 * side}, device_id_type=MESH,
        )

    def cols_source(par, side):
        return field.at[par, :, 1 + (lines - 1) * side]

    def slab_copy(par, side):
        return pltpu.make_async_remote_copy(
            src_ref=slab_out.at[par, side], dst_ref=slab_in.at[par, 1 - side],
            send_sem=slab_send.at[par, side], recv_sem=slab_recv.at[par, side],
            device_id={"slabs": s - 1 + 2 * side}, device_id_type=MESH,
        )

    def has(me, n, side):
        return me > 0 if side == 0 else me < n - 1

    def open_far():
        for span in spans(0):
            far_copy(0, *span).start()

    greet(has_far, {"rows": far_row})
    greet(core == 0, {"rows": near_row})

    @pl.when(jnp.logical_and(core == 0, has_far))
    def _():
        pl.semaphore_wait(barrier, 1)
        open_far()

    beside = jnp.int32(0)
    for axis, me, n in around:
        for there, other in ((me > 0, me - 1), (me < n - 1, me + 1)):
            greet(there, {"rows": r + 1 - core, axis: other})
            beside = beside + there.astype(jnp.int32)

    @pl.when(core == 1)
    def _():
        pl.semaphore_wait(barrier, 1 + has_far.astype(jnp.int32) + 2 * beside)

        @pl.when(has_far)
        def _():
            open_far()

    loads[0].start()

    @pl.when(core == 1)
    def _():
        pl.semaphore_signal(all_in, inc=1, device_id={"rows": near_row}, device_id_type=MESH)

    @pl.when(core == 0)
    def _():
        pl.semaphore_wait(all_in, 1)

    near_copy(0, tracer.at[layer(layers - 1)]).start()
    for side in (0, 1):
        @pl.when(has(q, cols_n, side))
        def _():
            cols_copy(0, side, tracer.at[:, (lines - 1) * side]).start()
    loads[1].start()

    for side in (0, 1):
        @pl.when(jnp.logical_not(has(q, cols_n, side)))
        def _():
            for par in (0, 1):
                field[par, :, (lines + 1) * side] = jnp.zeros((layers, depth, 128), jnp.float32)

        @pl.when(jnp.logical_not(has(s, slabs_n, side)))
        def _():
            for par in (0, 1):
                @pl.loop(0, layers)
                def _(i):
                    slab_in[par, side, i] = jnp.zeros((lines, 128), jnp.float32)

    @pl.when(jnp.logical_not(has_far))
    def _():
        for par in (0, 1):
            @pl.loop(0, lines)
            def _(j):
                far_in[par, j] = jnp.zeros((depth, 128), jnp.float32)

    loads[0].wait()

    @pl.loop(0, layers)
    def _(i):
        @pl.loop(0, lines)
        def _(j):
            slab_out[0, 0, i, pl.ds(j, 1), :] = field[0, i, j + 1, 0:1, :]
            slab_out[0, 1, i, pl.ds(j, 1), :] = field[0, i, j + 1, depth - 1:depth, :]

    for side in (0, 1):
        @pl.when(has(s, slabs_n, side))
        def _():
            slab_copy(0, side).start()
    loads[1].wait()

    row = lax.broadcasted_iota(jnp.int32, (8, 128), 0)

    def advance(t, d, start, count):
        par, last = t % 2, t == STEPS - 1
        here = layer(d)

        @pl.loop(start, start + count)
        def _(j):
            below = slab_in[par, 0, here, pl.ds(j, 1), :]
            above = slab_in[par, 1, here, pl.ds(j, 1), :]
            for k in range(tiles):
                part = pl.ds(8 * k, 8)
                mid = field[par, here, j + 1, part, :]
                if k == 0:
                    lower = jnp.where(row == 0, below, pltpu.roll(mid, 1, 0))
                else:
                    lower = field[par, here, j + 1, pl.ds(8 * k - 1, 8), :]
                if k == tiles - 1:
                    upper = jnp.where(row == 7, above, pltpu.roll(mid, 7, 0))
                else:
                    upper = field[par, here, j + 1, pl.ds(8 * k + 1, 8), :]
                outer = far_in[par, j, part, :] if d == 0 else field[par, layer(d - 1), j + 1, part, :]
                inner = near_in[par, j, part, :] if d == layers - 1 else field[par, layer(d + 1), j + 1, part, :]
                spread = (
                    (lower + upper)
                    + (field[par, here, j, part, :] + field[par, here, j + 2, part, :])
                    + (outer + inner)
                )
                crowd = out[here, j, part, :]
                new = 0.1 * spread + mid * (0.6 - 0.2 * (mid * crowd))
                if last:
                    out[here, j, part, :] = new
                else:
                    field[1 - par, here, j + 1, part, :] = new
                    if k == 0:
                        slab_out[1 - par, 0, here, pl.ds(j, 1), :] = new[0:1]
                    if k == tiles - 1:
                        slab_out[1 - par, 1, here, pl.ds(j, 1), :] = new[7:8]

    for t in range(STEPS):
        par, last = t % 2, t == STEPS - 1
        nxt = 1 - par
        near_copy(par, near_source(par)).wait_recv()
        for side in (0, 1):
            @pl.when(has(q, cols_n, 1 - side))
            def _():
                cols_copy(par, side, cols_source(par, side)).wait_recv()

            @pl.when(has(s, slabs_n, 1 - side))
            def _():
                slab_copy(par, side).wait_recv()
        if t > 0:
            near_copy(nxt, near_source(nxt)).wait_send()
            for side in (0, 1):
                @pl.when(has(q, cols_n, side))
                def _():
                    cols_copy(nxt, side, cols_source(nxt, side)).wait_send()

                @pl.when(has(s, slabs_n, side))
                def _():
                    slab_copy(nxt, side).wait_send()
        for d in range(layers - 1, 0, -1):
            advance(t, d, 0, lines)
        if not last:
            near_copy(nxt, near_source(nxt)).start()

        if t > 0:
            @pl.when(has_far)
            def _():
                for span in spans(t - 1):
                    far_copy(t - 1, *span).wait_send()

        for p, start, count in spans(t):
            @pl.when(has_far)
            def _():
                far_copy(t, p, start, count).wait_recv()

            advance(t, 0, start, count)
            if not last:
                @pl.when(has_far)
                def _():
                    for span in spans(t + 1):
                        if start < span[1] + span[2] <= start + count:
                            far_copy(t + 1, *span).start()
        if not last:
            for side in (0, 1):
                @pl.when(has(q, cols_n, side))
                def _():
                    cols_copy(nxt, side, cols_source(nxt, side)).start()

                @pl.when(has(s, slabs_n, side))
                def _():
                    slab_copy(nxt, side).start()

    par = (STEPS - 1) % 2
    near_copy(par, near_source(par)).wait_send()
    for side in (0, 1):
        @pl.when(has(q, cols_n, side))
        def _():
            cols_copy(par, side, cols_source(par, side)).wait_send()

        @pl.when(has(s, slabs_n, side))
        def _():
            slab_copy(par, side).wait_send()

    @pl.when(has_far)
    def _():
        for span in spans(STEPS - 1):
            far_copy(STEPS - 1, *span).wait_send()


def solution(mesh):
    sizes = tuple(mesh.shape[axis] for axis in ("rows", "cols", "slabs"))

    def on_device(tracer, crowding):
        layers, lines, depth, lanes = tracer.shape
        dma = pltpu.SemaphoreType.DMA
        return pl.pallas_call(
            functools.partial(kernel, sizes),
            out_shape=pltpu.VMEM(tracer.shape, jnp.float32),
            in_specs=[pl.BlockSpec(memory_space=pl.ANY)] * 2,
            out_specs=pl.BlockSpec(memory_space=pltpu.VMEM),
            scratch_shapes=[
                pltpu.VMEM((2, layers, lines + 2, depth, lanes), jnp.float32),
                pltpu.VMEM((2, lines, depth, lanes), jnp.float32),
                pltpu.VMEM((2, lines, depth, lanes), jnp.float32),
                pltpu.VMEM((2, 2, layers, lines, lanes), jnp.float32),
                pltpu.VMEM((2, 2, layers, lines, lanes), jnp.float32),
                pltpu.SemaphoreType.REGULAR,
                dma((2,)),
                dma((2, MOST)), dma((2, MOST)),
                dma((2,)), dma((2,)),
                dma((2, 2)), dma((2, 2)),
                dma((2, 2)), dma((2, 2)),
            ],
            compiler_params=pltpu.CompilerParams(
                collective_id=0, has_side_effects=True, vmem_limit_bytes=VMEM_LIMIT,
            ),
        )(tracer, crowding)

    placed = P("rows", "cols", "slabs", None)
    return jax.shard_map(on_device, mesh=mesh, in_specs=(placed, placed), out_specs=placed, check_vma=False)
```

```python
import functools

import jax
import jax.numpy as jnp
from jax import lax
from jax.experimental import pallas as pl
from jax.experimental.pallas import tpu as pltpu
from jax.sharding import PartitionSpec as P

STEPS = 4
PARTS = ((16, 32, 16), (16, 32, 16), (16, 32, 16), (16, 32, 10, 4, 1, 1))
MOST = max(map(len, PARTS))
MESH = pl.DeviceIdType.MESH
VMEM_LIMIT = 48 * 1024 * 1024


def kernel(sizes, tracer, crowding, out, field, far_in, near_in, slab_in, slab_out,
           all_in, load_sem, far_send, far_recv, near_send, near_recv,
           cols_send, cols_recv, slab_send, slab_recv):
    layers, lines, depth, _ = tracer.shape
    tiles = depth // 8
    rows_n, cols_n, slabs_n = sizes
    r, q, s = lax.axis_index("rows"), lax.axis_index("cols"), lax.axis_index("slabs")
    core = lax.rem(r, 2)
    step_up = 1 - 2 * core
    first = (layers - 1) * core

    def layer(d):
        return first + step_up * d

    far_row = r - step_up
    near_row = r + step_up
    has_far = jnp.logical_and(far_row >= 0, far_row < rows_n)
    around = (
        ("cols", q, cols_n),
        ("slabs", s, slabs_n),
    )

    def spans(t):
        start = 0
        for p, count in enumerate(PARTS[t]):
            yield p, start, count
            start += count

    loads = [
        pltpu.make_async_copy(tracer, field.at[0, :, pl.ds(1, lines)], load_sem.at[0]),
        pltpu.make_async_copy(crowding, out, load_sem.at[1]),
    ]

    barrier = pltpu.get_barrier_semaphore()

    def greet(there, target):
        @pl.when(there)
        def _():
            pl.semaphore_signal(barrier, inc=1, device_id=target, device_id_type=MESH)

    def far_copy(t, p, start, count):
        par = t % 2
        source = tracer.at[layer(0), pl.ds(start, count)] if t == 0 else field.at[par, layer(0), pl.ds(1 + start, count)]
        return pltpu.make_async_remote_copy(
            src_ref=source, dst_ref=far_in.at[par, pl.ds(start, count)],
            send_sem=far_send.at[par, p], recv_sem=far_recv.at[par, p],
            device_id={"rows": far_row}, device_id_type=MESH,
        )

    def near_copy(par, source):
        return pltpu.make_async_remote_copy(
            src_ref=source, dst_ref=near_in.at[par],
            send_sem=near_send.at[par], recv_sem=near_recv.at[par],
            device_id={"rows": near_row}, device_id_type=MESH,
        )

    def near_source(par):
        return field.at[par, layer(layers - 1), pl.ds(1, lines)]

    def cols_copy(par, side, source):
        return pltpu.make_async_remote_copy(
            src_ref=source, dst_ref=field.at[par, :, (lines + 1) * (1 - side)],
            send_sem=cols_send.at[par, side], recv_sem=cols_recv.at[par, side],
            device_id={"cols": q - 1 + 2 * side}, device_id_type=MESH,
        )

    def cols_source(par, side):
        return field.at[par, :, 1 + (lines - 1) * side]

    def slab_copy(par, side):
        return pltpu.make_async_remote_copy(
            src_ref=slab_out.at[par, side], dst_ref=slab_in.at[par, 1 - side],
            send_sem=slab_send.at[par, side], recv_sem=slab_recv.at[par, side],
            device_id={"slabs": s - 1 + 2 * side}, device_id_type=MESH,
        )

    def has(me, n, side):
        return me > 0 if side == 0 else me < n - 1

    def open_far():
        for span in spans(0):
            far_copy(0, *span).start()

    greet(has_far, {"rows": far_row})
    greet(core == 0, {"rows": near_row})

    @pl.when(jnp.logical_and(core == 0, has_far))
    def _():
        pl.semaphore_wait(barrier, 1)
        open_far()

    beside = jnp.int32(0)
    for axis, me, n in around:
        for there, other in ((me > 0, me - 1), (me < n - 1, me + 1)):
            greet(there, {"rows": r + 1 - core, axis: other})
            beside = beside + there.astype(jnp.int32)

    @pl.when(core == 1)
    def _():
        pl.semaphore_wait(barrier, 1 + has_far.astype(jnp.int32) + 2 * beside)

        @pl.when(has_far)
        def _():
            open_far()

    loads[0].start()

    @pl.when(core == 1)
    def _():
        pl.semaphore_signal(all_in, inc=1, device_id={"rows": near_row}, device_id_type=MESH)

    @pl.when(core == 0)
    def _():
        pl.semaphore_wait(all_in, 1)

    for side in (0, 1):
        @pl.when(has(q, cols_n, side))
        def _():
            cols_copy(0, side, tracer.at[:, (lines - 1) * side]).start()
    loads[1].start()

    for side in (0, 1):
        @pl.when(jnp.logical_not(has(q, cols_n, side)))
        def _():
            for par in (0, 1):
                field[par, :, (lines + 1) * side] = jnp.zeros((layers, depth, 128), jnp.float32)

        @pl.when(jnp.logical_not(has(s, slabs_n, side)))
        def _():
            for par in (0, 1):
                @pl.loop(0, layers)
                def _(i):
                    slab_in[par, side, i] = jnp.zeros((lines, 128), jnp.float32)

    @pl.when(jnp.logical_not(has_far))
    def _():
        for par in (0, 1):
            @pl.loop(0, lines)
            def _(j):
                far_in[par, j] = jnp.zeros((depth, 128), jnp.float32)

    loads[0].wait()

    @pl.loop(0, layers)
    def _(i):
        @pl.loop(0, lines)
        def _(j):
            slab_out[0, 0, i, pl.ds(j, 1), :] = field[0, i, j + 1, 0:1, :]
            slab_out[0, 1, i, pl.ds(j, 1), :] = field[0, i, j + 1, depth - 1:depth, :]

    for side in (0, 1):
        @pl.when(has(s, slabs_n, side))
        def _():
            slab_copy(0, side).start()
    near_copy(0, tracer.at[layer(layers - 1)]).start()
    loads[1].wait()

    row = lax.broadcasted_iota(jnp.int32, (8, 128), 0)

    def advance(t, d, start, count):
        par, last = t % 2, t == STEPS - 1
        here = layer(d)

        @pl.loop(start, start + count)
        def _(j):
            below = slab_in[par, 0, here, pl.ds(j, 1), :]
            above = slab_in[par, 1, here, pl.ds(j, 1), :]
            for k in range(tiles):
                part = pl.ds(8 * k, 8)
                mid = field[par, here, j + 1, part, :]
                if k == 0:
                    lower = jnp.where(row == 0, below, pltpu.roll(mid, 1, 0))
                else:
                    lower = field[par, here, j + 1, pl.ds(8 * k - 1, 8), :]
                if k == tiles - 1:
                    upper = jnp.where(row == 7, above, pltpu.roll(mid, 7, 0))
                else:
                    upper = field[par, here, j + 1, pl.ds(8 * k + 1, 8), :]
                outer = far_in[par, j, part, :] if d == 0 else field[par, layer(d - 1), j + 1, part, :]
                inner = near_in[par, j, part, :] if d == layers - 1 else field[par, layer(d + 1), j + 1, part, :]
                spread = (
                    (lower + upper)
                    + (field[par, here, j, part, :] + field[par, here, j + 2, part, :])
                    + (outer + inner)
                )
                crowd = out[here, j, part, :]
                new = 0.1 * spread + mid * (0.6 - 0.2 * (mid * crowd))
                if last:
                    out[here, j, part, :] = new
                else:
                    field[1 - par, here, j + 1, part, :] = new
                    if k == 0:
                        slab_out[1 - par, 0, here, pl.ds(j, 1), :] = new[0:1]
                    if k == tiles - 1:
                        slab_out[1 - par, 1, here, pl.ds(j, 1), :] = new[7:8]

    def settle():
        par = (STEPS - 1) % 2
        near_copy(par, near_source(par)).wait_send()
        for side in (0, 1):
            @pl.when(has(q, cols_n, side))
            def _():
                cols_copy(par, side, cols_source(par, side)).wait_send()

            @pl.when(has(s, slabs_n, side))
            def _():
                slab_copy(par, side).wait_send()

    for t in range(STEPS):
        par, last = t % 2, t == STEPS - 1
        nxt = 1 - par
        for side in (0, 1):
            @pl.when(has(q, cols_n, 1 - side))
            def _():
                cols_copy(par, side, cols_source(par, side)).wait_recv()

            @pl.when(has(s, slabs_n, 1 - side))
            def _():
                slab_copy(par, side).wait_recv()
        if t > 0:
            near_copy(nxt, near_source(nxt)).wait_send()
            for side in (0, 1):
                @pl.when(has(q, cols_n, side))
                def _():
                    cols_copy(nxt, side, cols_source(nxt, side)).wait_send()

                @pl.when(has(s, slabs_n, side))
                def _():
                    slab_copy(nxt, side).wait_send()
        for d in range(1, layers):
            if d == layers - 1:
                near_copy(par, near_source(par)).wait_recv()
            advance(t, d, 0, lines)
        if not last:
            near_copy(nxt, near_source(nxt)).start()

        if t > 0:
            @pl.when(has_far)
            def _():
                for span in spans(t - 1):
                    far_copy(t - 1, *span).wait_send()

        if last:
            settle()

        for p, start, count in spans(t):
            @pl.when(has_far)
            def _():
                far_copy(t, p, start, count).wait_recv()

            advance(t, 0, start, count)
            if not last:
                @pl.when(has_far)
                def _():
                    for span in spans(t + 1):
                        if start < span[1] + span[2] <= start + count:
                            far_copy(t + 1, *span).start()
        if not last:
            for side in (0, 1):
                @pl.when(has(q, cols_n, side))
                def _():
                    cols_copy(nxt, side, cols_source(nxt, side)).start()

                @pl.when(has(s, slabs_n, side))
                def _():
                    slab_copy(nxt, side).start()

    @pl.when(has_far)
    def _():
        for span in spans(STEPS - 1):
            far_copy(STEPS - 1, *span).wait_send()


def flush(source, out, sem):
    copies = [
        pltpu.make_async_copy(source.at[i, pl.ds(h, 32)], out.at[i, pl.ds(h, 32)], sem.at[i, h // 32])
        for i in range(source.shape[0]) for h in range(0, source.shape[1], 32)
    ]
    for copy in copies:
        copy.start()
    for copy in copies:
        copy.wait()


def solution(mesh):
    sizes = tuple(mesh.shape[axis] for axis in ("rows", "cols", "slabs"))

    def on_device(tracer, crowding):
        layers, lines, depth, lanes = tracer.shape
        dma = pltpu.SemaphoreType.DMA
        result = pl.pallas_call(
            functools.partial(kernel, sizes),
            out_shape=pltpu.VMEM(tracer.shape, jnp.float32),
            in_specs=[pl.BlockSpec(memory_space=pl.ANY)] * 2,
            out_specs=pl.BlockSpec(memory_space=pltpu.VMEM),
            scratch_shapes=[
                pltpu.VMEM((2, layers, lines + 2, depth, lanes), jnp.float32),
                pltpu.VMEM((2, lines, depth, lanes), jnp.float32),
                pltpu.VMEM((2, lines, depth, lanes), jnp.float32),
                pltpu.VMEM((2, 2, layers, lines, lanes), jnp.float32),
                pltpu.VMEM((2, 2, layers, lines, lanes), jnp.float32),
                pltpu.SemaphoreType.REGULAR,
                dma((2,)),
                dma((2, MOST)), dma((2, MOST)),
                dma((2,)), dma((2,)),
                dma((2, 2)), dma((2, 2)),
                dma((2, 2)), dma((2, 2)),
            ],
            compiler_params=pltpu.CompilerParams(
                collective_id=0, has_side_effects=True, vmem_limit_bytes=VMEM_LIMIT,
            ),
        )(tracer, crowding)
        return pl.pallas_call(
            flush,
            out_shape=jax.ShapeDtypeStruct(tracer.shape, jnp.float32),
            in_specs=[pl.BlockSpec(memory_space=pltpu.VMEM)],
            out_specs=pl.BlockSpec(memory_space=pl.ANY),
            scratch_shapes=[dma((layers, lines // 32))],
            compiler_params=pltpu.CompilerParams(vmem_limit_bytes=1024 * 1024),
        )(pltpu.with_memory_space_constraint(result, pltpu.VMEM))

    placed = P("rows", "cols", "slabs", None)
    return jax.shard_map(on_device, mesh=mesh, in_specs=(placed, placed), out_specs=placed, check_vma=False)
```

```python
import functools

import jax
import jax.numpy as jnp
from jax import lax
from jax.experimental import pallas as pl
from jax.experimental.pallas import tpu as pltpu
from jax.sharding import PartitionSpec as P

STEPS = 4
PARTS = ((16, 32, 16), (16, 32, 16), (16, 32, 16), (16, 32, 10, 4, 1, 1))
MOST = max(map(len, PARTS))
MESH = pl.DeviceIdType.MESH
VMEM_LIMIT = 48 * 1024 * 1024


def kernel(sizes, tracer, crowding, out, field, far_in, near_in, slab_in, slab_out,
           all_in, load_sem, far_send, far_recv, near_send, near_recv,
           cols_send, cols_recv, slab_send, slab_recv):
    layers, lines, depth, _ = tracer.shape
    tiles = depth // 8
    rows_n, cols_n, slabs_n = sizes
    r, q, s = lax.axis_index("rows"), lax.axis_index("cols"), lax.axis_index("slabs")
    core = lax.rem(r, 2)
    step_up = 1 - 2 * core
    first = (layers - 1) * core

    def layer(d):
        return first + step_up * d

    far_row = r - step_up
    near_row = r + step_up
    has_far = jnp.logical_and(far_row >= 0, far_row < rows_n)
    around = (
        ("cols", q, cols_n),
        ("slabs", s, slabs_n),
    )

    def spans(t):
        start = 0
        for p, count in enumerate(PARTS[t]):
            yield p, start, count
            start += count

    loads = [
        pltpu.make_async_copy(tracer, field.at[0, :, pl.ds(1, lines)], load_sem.at[0]),
        pltpu.make_async_copy(crowding, out, load_sem.at[1]),
    ]

    barrier = pltpu.get_barrier_semaphore()

    def greet(there, target):
        @pl.when(there)
        def _():
            pl.semaphore_signal(barrier, inc=1, device_id=target, device_id_type=MESH)

    def far_copy(t, p, start, count):
        par = t % 2
        source = tracer.at[layer(0), pl.ds(start, count)] if t == 0 else field.at[par, layer(0), pl.ds(1 + start, count)]
        return pltpu.make_async_remote_copy(
            src_ref=source, dst_ref=far_in.at[par, pl.ds(start, count)],
            send_sem=far_send.at[par, p], recv_sem=far_recv.at[par, p],
            device_id={"rows": far_row}, device_id_type=MESH,
        )

    def near_copy(par, source):
        return pltpu.make_async_remote_copy(
            src_ref=source, dst_ref=near_in.at[par],
            send_sem=near_send.at[par], recv_sem=near_recv.at[par],
            device_id={"rows": near_row}, device_id_type=MESH,
        )

    def near_source(par):
        return field.at[par, layer(layers - 1), pl.ds(1, lines)]

    def cols_copy(par, side, source):
        return pltpu.make_async_remote_copy(
            src_ref=source, dst_ref=field.at[par, :, (lines + 1) * (1 - side)],
            send_sem=cols_send.at[par, side], recv_sem=cols_recv.at[par, side],
            device_id={"cols": q - 1 + 2 * side}, device_id_type=MESH,
        )

    def cols_source(par, side):
        return field.at[par, :, 1 + (lines - 1) * side]

    def slab_copy(par, side):
        return pltpu.make_async_remote_copy(
            src_ref=slab_out.at[par, side], dst_ref=slab_in.at[par, 1 - side],
            send_sem=slab_send.at[par, side], recv_sem=slab_recv.at[par, side],
            device_id={"slabs": s - 1 + 2 * side}, device_id_type=MESH,
        )

    def has(me, n, side):
        return me > 0 if side == 0 else me < n - 1

    def open_far():
        for span in spans(0):
            far_copy(0, *span).start()

    greet(has_far, {"rows": far_row})
    greet(core == 0, {"rows": near_row})

    @pl.when(jnp.logical_and(core == 0, has_far))
    def _():
        pl.semaphore_wait(barrier, 1)
        open_far()

    beside = jnp.int32(0)
    for axis, me, n in around:
        for there, other in ((me > 0, me - 1), (me < n - 1, me + 1)):
            greet(there, {"rows": r + 1 - core, axis: other})
            beside = beside + there.astype(jnp.int32)

    @pl.when(core == 1)
    def _():
        pl.semaphore_wait(barrier, 1 + has_far.astype(jnp.int32) + 2 * beside)

        @pl.when(has_far)
        def _():
            open_far()

    loads[0].start()

    @pl.when(core == 1)
    def _():
        pl.semaphore_signal(all_in, inc=1, device_id={"rows": near_row}, device_id_type=MESH)

    @pl.when(core == 0)
    def _():
        pl.semaphore_wait(all_in, 1)

    loads[1].start()

    for side in (0, 1):
        @pl.when(jnp.logical_not(has(q, cols_n, side)))
        def _():
            for par in (0, 1):
                field[par, :, (lines + 1) * side] = jnp.zeros((layers, depth, 128), jnp.float32)

        @pl.when(jnp.logical_not(has(s, slabs_n, side)))
        def _():
            for par in (0, 1):
                @pl.loop(0, layers)
                def _(i):
                    slab_in[par, side, i] = jnp.zeros((lines, 128), jnp.float32)

    @pl.when(jnp.logical_not(has_far))
    def _():
        for par in (0, 1):
            @pl.loop(0, lines)
            def _(j):
                far_in[par, j] = jnp.zeros((depth, 128), jnp.float32)

    loads[0].wait()
    for side in (0, 1):
        @pl.when(has(q, cols_n, side))
        def _():
            cols_copy(0, side, tracer.at[:, (lines - 1) * side]).start()

    @pl.loop(0, layers)
    def _(i):
        @pl.loop(0, lines)
        def _(j):
            slab_out[0, 0, i, pl.ds(j, 1), :] = field[0, i, j + 1, 0:1, :]
            slab_out[0, 1, i, pl.ds(j, 1), :] = field[0, i, j + 1, depth - 1:depth, :]

    for side in (0, 1):
        @pl.when(has(s, slabs_n, side))
        def _():
            slab_copy(0, side).start()
    near_copy(0, tracer.at[layer(layers - 1)]).start()
    loads[1].wait()

    row = lax.broadcasted_iota(jnp.int32, (8, 128), 0)

    def advance(t, d, start, count):
        par, last = t % 2, t == STEPS - 1
        here = layer(d)

        @pl.loop(start, start + count)
        def _(j):
            below = slab_in[par, 0, here, pl.ds(j, 1), :]
            above = slab_in[par, 1, here, pl.ds(j, 1), :]
            for k in range(tiles):
                part = pl.ds(8 * k, 8)
                mid = field[par, here, j + 1, part, :]
                if k == 0:
                    lower = jnp.where(row == 0, below, pltpu.roll(mid, 1, 0))
                else:
                    lower = field[par, here, j + 1, pl.ds(8 * k - 1, 8), :]
                if k == tiles - 1:
                    upper = jnp.where(row == 7, above, pltpu.roll(mid, 7, 0))
                else:
                    upper = field[par, here, j + 1, pl.ds(8 * k + 1, 8), :]
                outer = far_in[par, j, part, :] if d == 0 else field[par, layer(d - 1), j + 1, part, :]
                inner = near_in[par, j, part, :] if d == layers - 1 else field[par, layer(d + 1), j + 1, part, :]
                spread = (
                    (lower + upper)
                    + (field[par, here, j, part, :] + field[par, here, j + 2, part, :])
                    + (outer + inner)
                )
                crowd = out[here, j, part, :]
                new = 0.1 * spread + mid * (0.6 - 0.2 * (mid * crowd))
                if last:
                    out[here, j, part, :] = new
                else:
                    field[1 - par, here, j + 1, part, :] = new
                    if k == 0:
                        slab_out[1 - par, 0, here, pl.ds(j, 1), :] = new[0:1]
                    if k == tiles - 1:
                        slab_out[1 - par, 1, here, pl.ds(j, 1), :] = new[7:8]

    for t in range(STEPS):
        par, last = t % 2, t == STEPS - 1
        nxt = 1 - par
        for side in (0, 1):
            @pl.when(has(q, cols_n, 1 - side))
            def _():
                cols_copy(par, side, cols_source(par, side)).wait_recv()

            @pl.when(has(s, slabs_n, 1 - side))
            def _():
                slab_copy(par, side).wait_recv()
        if t > 0:
            near_copy(nxt, near_source(nxt)).wait_send()
            for side in (0, 1):
                @pl.when(has(q, cols_n, side))
                def _():
                    cols_copy(nxt, side, cols_source(nxt, side)).wait_send()

                @pl.when(has(s, slabs_n, side))
                def _():
                    slab_copy(nxt, side).wait_send()
        for d in range(1, layers):
            if d == layers - 1:
                near_copy(par, near_source(par)).wait_recv()
            advance(t, d, 0, lines)
        if not last:
            near_copy(nxt, near_source(nxt)).start()

        if t > 0:
            @pl.when(has_far)
            def _():
                for span in spans(t - 1):
                    far_copy(t - 1, *span).wait_send()

        for p, start, count in spans(t):
            @pl.when(has_far)
            def _():
                far_copy(t, p, start, count).wait_recv()

            advance(t, 0, start, count)
            if not last:
                @pl.when(has_far)
                def _():
                    for span in spans(t + 1):
                        if start < span[1] + span[2] <= start + count:
                            far_copy(t + 1, *span).start()
        if not last:
            for side in (0, 1):
                @pl.when(has(q, cols_n, side))
                def _():
                    cols_copy(nxt, side, cols_source(nxt, side)).start()

                @pl.when(has(s, slabs_n, side))
                def _():
                    slab_copy(nxt, side).start()

    par = (STEPS - 1) % 2
    near_copy(par, near_source(par)).wait_send()
    for side in (0, 1):
        @pl.when(has(q, cols_n, side))
        def _():
            cols_copy(par, side, cols_source(par, side)).wait_send()

        @pl.when(has(s, slabs_n, side))
        def _():
            slab_copy(par, side).wait_send()

    @pl.when(has_far)
    def _():
        for span in spans(STEPS - 1):
            far_copy(STEPS - 1, *span).wait_send()


def solution(mesh):
    sizes = tuple(mesh.shape[axis] for axis in ("rows", "cols", "slabs"))

    def on_device(tracer, crowding):
        layers, lines, depth, lanes = tracer.shape
        dma = pltpu.SemaphoreType.DMA
        return pl.pallas_call(
            functools.partial(kernel, sizes),
            out_shape=pltpu.VMEM(tracer.shape, jnp.float32),
            in_specs=[pl.BlockSpec(memory_space=pl.ANY)] * 2,
            out_specs=pl.BlockSpec(memory_space=pltpu.VMEM),
            scratch_shapes=[
                pltpu.VMEM((2, layers, lines + 2, depth, lanes), jnp.float32),
                pltpu.VMEM((2, lines, depth, lanes), jnp.float32),
                pltpu.VMEM((2, lines, depth, lanes), jnp.float32),
                pltpu.VMEM((2, 2, layers, lines, lanes), jnp.float32),
                pltpu.VMEM((2, 2, layers, lines, lanes), jnp.float32),
                pltpu.SemaphoreType.REGULAR,
                dma((2,)),
                dma((2, MOST)), dma((2, MOST)),
                dma((2,)), dma((2,)),
                dma((2, 2)), dma((2, 2)),
                dma((2, 2)), dma((2, 2)),
            ],
            compiler_params=pltpu.CompilerParams(
                collective_id=0, has_side_effects=True, vmem_limit_bytes=VMEM_LIMIT,
            ),
        )(tracer, crowding)

    placed = P("rows", "cols", "slabs", None)
    return jax.shard_map(on_device, mesh=mesh, in_specs=(placed, placed), out_specs=placed, check_vma=False)
```
